512 devices in a mesh: env: 64 (over x, z), feat: 8 (over y, core).
Axes of the slice: x: 4, y: 4, z: 16, core: 2. Of those that a mesh axis runs over, the one named last changes fastest.
Arguments:
- observations: bfloat16 [32768, 8192], P('env', 'feat'), may hold values from -256 to 256, as said below
- prior_count: int32 [8192], P('feat'), may hold values from 8192 to 131071
- prior_mean: float32 [8192], P('feat'), may hold values from -12 to 12
- prior_var: float32 [8192], P('feat'), may hold values from 0.5 to 40
- policy_weight: bfloat16 [8192, 4096], P('feat', 'env'), may hold values from -0.0625 to 0.0625
Outputs:
- run_mean: float32 [8192], P('feat')
- run_var: float32 [8192], P('feat')
- logits: bfloat16 [32768, 4096], P('env', 'feat')
The draws below stay inside these ranges and needn't reach their ends.
Inputs may be any that keep to these rules, and one draw needn't show every extreme that they name: observations have per-environment scales and per-feature offsets.
All inputs are finite; a program needn't handle non-finite values.
Results may differ from the reference program's by a relative error of at most 0.013.
Values may be sent and summed in bfloat16 or wider, within the bound.
No kernel may reach another device: no remote copies, remote signals or barrier semaphores. Data moves between devices by JAX's collectives and lax.ppermute only.
A program may use at most 64 MiB of HBM per device.

```python
import math
import jax
import jax.numpy as jnp
from jax import lax

D = 8192
H = 4096
TOKENS = 32768
N_FEAT = 8


def draw_observations(key, part):
    keys = jax.random.split(key, 4)
    rows = jnp.arange(TOKENS, dtype=jnp.float32)
    row_scale = jnp.exp(jax.random.uniform(keys[0], (TOKENS,), jnp.float32) * jnp.log(10.0)) * jnp.exp(jnp.log(3.0) * rows / TOKENS)
    feature_scale = jnp.exp(jax.random.uniform(keys[1], (D,), jnp.float32, -0.7, 0.7))
    offset = jax.random.normal(keys[2], (D,), jnp.float32)
    noise = jnp.clip(jax.random.normal(keys[3], (TOKENS, D), jnp.float32), -4.0, 4.0)
    values = offset[None, :] + row_scale[:, None] * feature_scale[None, :] * noise
    return jnp.clip(values, -256.0, 256.0).astype(jnp.bfloat16)


def with_ends(drawn, own_key, least, largest):
    dims = drawn.shape
    spot = [jax.random.randint(jax.random.fold_in(own_key, axis), (), 0, dims[axis]) for axis in range(len(dims))]
    drawn = drawn.at[tuple(spot)].set(least)
    longest = dims.index(max(dims))
    spot[longest] = (spot[longest] + 1) % dims[longest]
    return drawn.at[tuple(spot)].set(largest)


def level_of(key, shape, cuts, least, high):
    level, own = 1.0, jax.random.fold_in(key, 6)
    for dim, parts in cuts:
        draws = jnp.exp(jax.random.uniform(jax.random.fold_in(own, dim), (parts,), jnp.float32, least / len(cuts), high / len(cuts)))
        level = level * jnp.repeat(draws, shape[dim] // parts).reshape([-1 if axis == dim else 1 for axis in range(len(shape))])
    return level


def bell_draw(own_key, extent, spread, reach, shards=(), held_as=jnp.bfloat16):
    values = jax.random.normal(own_key, extent, jnp.float32) * spread
    if len(shards) > 0:
        values = level_of(own_key, extent, shards, -0.22, 0.18) * values
    return jnp.clip(values, min=-reach, max=reach).astype(held_as)


def setup_inputs(seed: int = 0) -> dict:
    key_of = jax.random.split(jax.random.key(seed), 6)
    observations = draw_observations(jax.random.fold_in(key_of[5], 71), 0)
    prior_count = with_ends(jax.random.randint(key_of[1], (D,), TOKENS // 4, 4 * TOKENS), jax.random.fold_in(key_of[1], 1), TOKENS // 4, (4 * TOKENS) - 1).astype(jnp.int32)
    prior_mean = bell_draw(key_of[2], (D,), 2.0, 12.0, ((0, 8),), jnp.float32)
    prior_var = jnp.clip(jnp.exp(math.log(40.0) - 4.3820266 * jax.random.uniform(key_of[3], (D,), jnp.float32) ** level_of(key_of[3], (D,), ((0, 8),), -0.2, 0.2)), 0.5, 40.0)
    policy_weight = bell_draw(key_of[4], (D, H), D ** -0.5, 0.0625, ((0, 8), (1, 64)))
    return dict(observations=observations, prior_count=prior_count, prior_mean=prior_mean, prior_var=prior_var, policy_weight=policy_weight)


def reference(observations, prior_count, prior_mean, prior_var, policy_weight):
    values = observations.astype(jnp.float32)
    batch_mean = lax.optimization_barrier(jnp.mean(values, axis=0))
    batch_m2 = lax.optimization_barrier(jnp.sum((values - batch_mean) ** 2, axis=0))
    count = prior_count.astype(jnp.float32)
    batch_n = jnp.float32(TOKENS)
    total = count + batch_n
    delta = batch_mean - prior_mean
    run_mean = prior_mean + delta * batch_n / total
    run_var = (prior_var * count + batch_m2 + delta * delta * count * batch_n / total) / total
    normalized = jnp.clip((values - run_mean) / jnp.sqrt(run_var + 1e-05), -5.0, 5.0).astype(jnp.bfloat16)
    width = D // N_FEAT
    summed = jnp.zeros((TOKENS, H), jnp.float32)
    for block in range(N_FEAT):
        left = normalized[:, block * width:(block + 1) * width].astype(jnp.float32)
        right = policy_weight[block * width:(block + 1) * width].astype(jnp.float32)
        partial_block = jnp.dot(left, right, precision=lax.Precision.HIGHEST).astype(jnp.bfloat16)
        summed = summed + partial_block.astype(jnp.float32)
    return (run_mean, run_var, summed.astype(jnp.bfloat16))
```

```python
import jax
import jax.numpy as jnp
import numpy as np
from jax import lax
from jax.sharding import Mesh
from jax.sharding import PartitionSpec as P

ENV = ("x", "zh", "zl")
Z = ("zh", "zl")
PLANE = ("x", "y")
FEAT = ("y", "c")
SIZES = {"x": 4, "zh": 8, "zl": 2, "y": 4, "c": 2}


def shift(value, axes, by):
    n = int(np.prod([SIZES[a] for a in ((axes,) if isinstance(axes, str) else axes)]))
    return lax.ppermute(value, axes, [(i, (i + by) % n) for i in range(n)])


def shards(observations, prior_count, prior_mean, prior_var, policy_weight):
    rows = observations.shape[0]
    x, zl, y, c = (lax.axis_index(a) for a in ("x", "zl", "y", "c"))
    batch_n = jnp.float32(rows * lax.axis_size(ENV))

    weight_a = lax.all_gather(policy_weight.T, "zh", axis=0, tiled=True)

    blocks = [
        observations,
        shift(observations, "x", -1),
        shift(observations, "x", 2),
        shift(observations, "x", 1),
    ]

    off = observations.astype(jnp.float32) - prior_mean
    sums = jnp.stack([jnp.sum(off, axis=0), jnp.sum(off * off, axis=0)])
    sums = jnp.broadcast_to(sums.reshape(1, 16, 128), (lax.axis_size(ENV), 16, 128))
    sums = lax.all_to_all(sums, ENV, 0, 0).sum(axis=0).reshape(2, -1)
    count = prior_count.astype(jnp.float32)
    total = count + batch_n
    run_mean = prior_mean + sums[0] / total
    run_var = (prior_var * count + (sums[1] - sums[0] * sums[0] / total)) / total
    scale = 1.0 / jnp.sqrt(run_var + 1e-05)

    normal = jnp.concatenate(blocks, axis=0).astype(jnp.float32)
    normal = jnp.clip((normal - run_mean) * scale, -5.0, 5.0).astype(jnp.bfloat16)

    half = weight_a.shape[0] // 2
    weight_b = jnp.concatenate(
        [shift(weight_a[:half], Z, 1), shift(weight_a[half:], Z, -1)], axis=0
    )

    def times(weight):
        out = lax.dot_general(
            normal, weight, (((1,), (1,)), ((), ())), preferred_element_type=jnp.float32
        )
        low, high = out[:, :half], out[:, half:]
        keep = jnp.where(c == 0, low, high)
        send = jnp.where(c == 0, high, low).astype(jnp.bfloat16)
        other = lax.ppermute(send, "c", [(0, 1), (1, 0)])
        return (keep + other.astype(jnp.float32)).astype(jnp.bfloat16)

    part = jnp.concatenate([times(weight_a), times(weight_b)], axis=1).reshape(4, rows, -1)
    arrived = []
    for k in range(4):
        piece = lax.dynamic_index_in_dim(part, (y + k - x) % 4, 0, keepdims=False)
        pairs = [(4 * a + b, 4 * ((b + k) % 4) + a) for a in range(4) for b in range(4)]
        arrived.append(lax.ppermute(piece, PLANE, pairs))
    summed = sum(a.astype(jnp.float32) for a in arrived).astype(jnp.bfloat16)
    a, b = summed[:, :half], summed[:, half:]
    even = jnp.where(zl == 0, a, b).reshape(rows, 4, 1, -1)
    odd = jnp.where(zl == 0, b, a).reshape(rows, 4, 1, -1)
    logits = jnp.concatenate([even, odd], axis=2).reshape(rows, -1)
    return (run_mean, run_var, logits)


def solution(mesh):
    torus = Mesh(mesh.devices.reshape(*SIZES.values()), tuple(SIZES))
    in_specs = (P(ENV, FEAT), P(FEAT), P(FEAT), P(FEAT), P(FEAT, ENV))
    out_specs = (P(FEAT), P(FEAT), P(ENV, FEAT))
    return jax.shard_map(
        shards, mesh=torus, in_specs=in_specs, out_specs=out_specs, check_vma=False
    )
```

```python
import functools

import jax
import jax.numpy as jnp
import numpy as np
from jax import lax
from jax.experimental import pallas as pl
from jax.experimental.pallas import tpu as pltpu
from jax.sharding import Mesh
from jax.sharding import PartitionSpec as P

ENV = ("x", "z")
FEAT = ("y", "c")
SIZES = {"x": 4, "z": 16, "y": 4, "c": 2}
AXES = tuple(SIZES)
SHAPE = tuple(SIZES.values())

BLOCKS = (0, 1, 3, 2)


def fetch(value, source):
    pairs = []
    for to in range(int(np.prod(SHAPE))):
        at = source(*(int(k) for k in np.unravel_index(to, SHAPE)))
        at = tuple(k % n for k, n in zip(at, SHAPE))
        pairs.append((int(np.ravel_multi_index(at, SHAPE)), to))
    return lax.ppermute(value, AXES, pairs)


def along_x(value, by):
    return fetch(value, lambda x, z, y, c: (x + by, z, y, c))


def holder(x, q):
    q = q % 16
    return q % 4, 4 * (q // 4) + x


def across(value):
    return fetch(value, lambda x, z, y, c: (x, z, y, 1 - c))


def along_z(value, by):
    return fetch(value, lambda x, z, y, c: (x, z + (by if c else -by), y, c))


def sum_over(value, axis):
    copies = jnp.broadcast_to(value[None], (lax.axis_size(axis), *value.shape))
    copies = lax.all_to_all(copies, axis, 0, 0)
    return copies.sum(axis=0)


def normal_kernel(mean, factor, *refs):
    for k, block in enumerate(refs[:-1]):
        value = (block[...].astype(jnp.float32) - mean[...]) * factor[...]
        refs[-1][k] = jnp.clip(value, -5.0, 5.0).astype(jnp.bfloat16)


def normal(blocks, mean, factor):
    rows, depth = blocks[0].shape
    tile = rows // 4
    line = pl.BlockSpec((1, depth), lambda k: (0, 0))
    return pl.pallas_call(
        normal_kernel,
        out_shape=jax.ShapeDtypeStruct((4, rows, depth), jnp.bfloat16),
        grid=(rows // tile,),
        in_specs=[line, line] + [pl.BlockSpec((tile, depth), lambda k: (k, 0))] * 4,
        out_specs=pl.BlockSpec((4, tile, depth), lambda k: (0, k, 0)),
        compiler_params=pltpu.CompilerParams(vmem_limit_bytes=12 * 1024 * 1024),
        cost_estimate=pl.CostEstimate(
            flops=20 * rows * depth, bytes_accessed=16 * rows * depth, transcendentals=0
        ),
    )(mean[None], factor[None], *blocks)


def product_kernel(side, order, places, *refs):
    slots, value = refs[:8], refs[8]
    *before, out, weight, held, sem, held_sem = refs[9:]
    step = pl.program_id(0)
    width = slots[0].shape[0] // 2

    def copy(k):
        return pltpu.make_async_copy(
            slots[k].at[pl.ds(side * width, width)],
            weight.at[pl.ds(pl.multiple_of(places[k] * width, width), width)],
            sem.at[k],
        )

    def fetched(k):
        return pltpu.make_async_copy(value.at[k], held.at[k], held_sem.at[k])

    @pl.when(step == 0)
    def _():
        for k in range(8):
            copy(k).start()
        for k in range(4):
            fetched(k).start()
        for k in range(8):
            copy(k).wait()

    fetched(step).wait()
    total = lax.dot_general(
        weight[...], held[step], (((1,), (1,)), ((), ())), preferred_element_type=jnp.float32
    )
    if before:
        total = total + before[0][0].astype(jnp.float32)
    out[0] = total.astype(out.dtype)


def product(side, order, places, slots, value, *before):
    _, rows, depth = value.shape
    columns = 4 * slots[0].shape[0]
    to = (lambda k, order, *_: (order[k], 0, 0)) if before else (lambda k, *_: (k, 0, 0))
    return pl.pallas_call(
        functools.partial(product_kernel, side),
        out_shape=jax.ShapeDtypeStruct((4, columns, rows), jnp.bfloat16),
        grid_spec=pltpu.PrefetchScalarGridSpec(
            num_scalar_prefetch=2,
            grid=(4,),
            in_specs=[pl.BlockSpec(memory_space=pl.ANY)] * 9
            + [pl.BlockSpec((1, columns, rows), lambda k, *_: (k, 0, 0))] * len(before),
            out_specs=pl.BlockSpec((1, columns, rows), to),
            scratch_shapes=[
                pltpu.VMEM((columns, depth), jnp.bfloat16),
                pltpu.VMEM(value.shape, jnp.bfloat16),
                pltpu.SemaphoreType.DMA((8,)),
                pltpu.SemaphoreType.DMA((4,)),
            ],
        ),
        compiler_params=pltpu.CompilerParams(vmem_limit_bytes=16 * 1024 * 1024),
        cost_estimate=pl.CostEstimate(
            flops=8 * columns * rows * depth, bytes_accessed=9 << 20, transcendentals=0
        ),
    )(order, places, *slots, value, *before)


def step(observations, prior_count, prior_mean, prior_var, policy_weight):
    rows, _ = observations.shape
    x, z, y, c = (lax.axis_index(a) for a in AXES)
    batch_n = jnp.float32(rows * lax.axis_size(ENV))

    own = policy_weight.T
    slots = [
        jnp.concatenate(
            [
                fetch(own, lambda x, z, y, c: (*holder(x, z + c), y, c)),
                fetch(own, lambda x, z, y, c: (*holder(x, z + c), y, 1 - c)),
            ],
            axis=0,
        )
    ]
    slots.append(along_z(slots[0], 1))
    for k in range(2, 8):
        slots.append(along_z(slots[k - 2], 2))

    off = observations.astype(jnp.float32) - prior_mean
    sums = jnp.stack([jnp.sum(off, axis=0), jnp.sum(off * off, axis=0)])
    sums = sum_over(sums.reshape(16, 128), "x")
    sums = sum_over(sums, "z").reshape(2, -1)
    count = prior_count.astype(jnp.float32)
    total = count + batch_n
    run_mean = prior_mean + sums[0] / total
    run_var = (prior_var * count + (sums[1] - sums[0] * sums[0] / total)) / total
    scale = 1.0 / jnp.sqrt(run_var + 1e-05)

    blocks = [along_x(observations, by) if by else observations for by in BLOCKS]
    q = jnp.where(c == 0, z - jnp.arange(8), z + 1 + jnp.arange(8)) % 16
    places = (2 * (q % 4) + (q // 4) % 2).astype(jnp.int32)
    order = ((x + jnp.array(BLOCKS)) % 4).astype(jnp.int32)
    value = normal(blocks, run_mean, scale)
    part = product(0, order, places, slots, value)
    value = across(value)
    part = product(1, order, places, slots, value, part)

    part = lax.all_to_all(part.reshape(16, -1, rows), ("x", "y"), 0, 0)
    summed = part.reshape(4, 4, 2, -1, rows).astype(jnp.float32).sum(axis=1)
    summed = summed.astype(jnp.bfloat16)
    other = across(summed)
    sides = []
    for half in range(2):
        q = 4 * (2 * c + half) + y
        mine = jnp.where(c == 0, z - q, q - z - 1) % 16 < 8
        sides.append(jnp.where(mine, summed[:, half], other[:, half]))
    logits = jnp.concatenate(sides, axis=0).reshape(-1, rows).T
    return (run_mean, run_var, logits)


def solution(mesh):
    torus = Mesh(mesh.devices.reshape(SHAPE), AXES)
    in_specs = (P(ENV, FEAT), P(FEAT), P(FEAT), P(FEAT), P(FEAT, ENV))
    out_specs = (P(FEAT), P(FEAT), P(ENV, FEAT))
    return jax.shard_map(step, mesh=torus, in_specs=in_specs, out_specs=out_specs, check_vma=False)
```

```python
import functools

import jax
import jax.numpy as jnp
import numpy as np
from jax import lax
from jax.experimental import pallas as pl
from jax.experimental.pallas import tpu as pltpu
from jax.sharding import Mesh
from jax.sharding import PartitionSpec as P

ENV = ("x", "z")
FEAT = ("y", "c")
SIZES = {"x": 4, "z": 16, "y": 4, "c": 2}
AXES = tuple(SIZES)
SHAPE = tuple(SIZES.values())

BLOCKS = (0, 1, 3, 2)


def fetch(value, source):
    pairs = []
    for to in range(int(np.prod(SHAPE))):
        at = source(*(int(k) for k in np.unravel_index(to, SHAPE)))
        at = tuple(k % n for k, n in zip(at, SHAPE))
        pairs.append((int(np.ravel_multi_index(at, SHAPE)), to))
    return lax.ppermute(value, AXES, pairs)


def along_x(value, by):
    return fetch(value, lambda x, z, y, c: (x + by, z, y, c))


def holder(x, q):
    q = q % 16
    return q % 4, 4 * (q // 4) + x


def across(value):
    return fetch(value, lambda x, z, y, c: (x, z, y, 1 - c))


def along_z(value, by):
    return fetch(value, lambda x, z, y, c: (x, z + (by if c else -by), y, c))


def sum_over(value, axis):
    copies = jnp.broadcast_to(value[None], (lax.axis_size(axis), *value.shape))
    copies = lax.all_to_all(copies, axis, 0, 0)
    return copies.sum(axis=0)


def normal_kernel(mean, factor, *refs):
    for k, block in enumerate(refs[:-1]):
        value = (block[...].astype(jnp.float32) - mean[...]) * factor[...]
        refs[-1][k] = jnp.clip(value, -5.0, 5.0).astype(jnp.bfloat16)


def normal(blocks, mean, factor):
    rows, depth = blocks[0].shape
    tile = rows // 2
    line = pl.BlockSpec((1, depth), lambda k: (0, 0))
    return pl.pallas_call(
        normal_kernel,
        out_shape=jax.ShapeDtypeStruct((4, rows, depth), jnp.bfloat16),
        grid=(rows // tile,),
        in_specs=[line, line] + [pl.BlockSpec((tile, depth), lambda k: (k, 0))] * 4,
        out_specs=pl.BlockSpec((4, tile, depth), lambda k: (0, k, 0)),
        compiler_params=pltpu.CompilerParams(vmem_limit_bytes=24 * 1024 * 1024),
        cost_estimate=pl.CostEstimate(
            flops=20 * rows * depth, bytes_accessed=16 * rows * depth, transcendentals=0
        ),
    )(mean[None], factor[None], *blocks)


def product_kernel(side, order, places, *refs):
    slots, value = refs[:8], refs[8]
    *before, out, weight, held, sem, held_sem = refs[9:]
    step = pl.program_id(0)
    width = slots[0].shape[0] // 2

    def copy(k):
        return pltpu.make_async_copy(
            slots[k].at[pl.ds(side * width, width)],
            weight.at[pl.ds(pl.multiple_of(places[k] * width, width), width)],
            sem.at[k],
        )

    def fetched(k):
        return pltpu.make_async_copy(value.at[k], held.at[k], held_sem.at[k])

    @pl.when(step == 0)
    def _():
        for k in range(8):
            copy(k).start()
        for k in range(4):
            fetched(k).start()
        for k in range(8):
            copy(k).wait()

    for at in range(out.shape[0]):
        k = step * out.shape[0] + at
        fetched(k).wait()
        total = lax.dot_general(
            weight[...], held[k], (((1,), (1,)), ((), ())), preferred_element_type=jnp.float32
        )
        if before:
            total = total + before[0][0].astype(jnp.float32)
        out[at] = total.astype(out.dtype)


def product(side, order, places, slots, value, *before):
    _, rows, depth = value.shape
    columns = 4 * slots[0].shape[0]
    each = 1 if before else 2
    to = (lambda k, order, *_: (order[k], 0, 0)) if before else (lambda k, *_: (k, 0, 0))
    return pl.pallas_call(
        functools.partial(product_kernel, side),
        out_shape=jax.ShapeDtypeStruct((4, columns, rows), jnp.bfloat16),
        grid_spec=pltpu.PrefetchScalarGridSpec(
            num_scalar_prefetch=2,
            grid=(4 // each,),
            in_specs=[pl.BlockSpec(memory_space=pl.ANY)] * 9
            + [pl.BlockSpec((1, columns, rows), lambda k, *_: (k, 0, 0))] * len(before),
            out_specs=pl.BlockSpec((each, columns, rows), to),
            scratch_shapes=[
                pltpu.VMEM((columns, depth), jnp.bfloat16),
                pltpu.VMEM(value.shape, jnp.bfloat16),
                pltpu.SemaphoreType.DMA((8,)),
                pltpu.SemaphoreType.DMA((4,)),
            ],
        ),
        compiler_params=pltpu.CompilerParams(vmem_limit_bytes=16 * 1024 * 1024),
        cost_estimate=pl.CostEstimate(
            flops=8 * columns * rows * depth, bytes_accessed=9 << 20, transcendentals=0
        ),
    )(order, places, *slots, value, *before)


def step(observations, prior_count, prior_mean, prior_var, policy_weight):
    rows, _ = observations.shape
    x, z, y, c = (lax.axis_index(a) for a in AXES)
    batch_n = jnp.float32(rows * lax.axis_size(ENV))

    own = policy_weight.T
    slots = [
        jnp.concatenate(
            [
                fetch(own, lambda x, z, y, c: (*holder(x, z + c), y, c)),
                fetch(own, lambda x, z, y, c: (*holder(x, z + c), y, 1 - c)),
            ],
            axis=0,
        )
    ]
    slots.append(along_z(slots[0], 1))
    for k in range(2, 8):
        slots.append(along_z(slots[k - 2], 2))

    off = observations.astype(jnp.float32) - prior_mean
    sums = jnp.stack([jnp.sum(off, axis=0), jnp.sum(off * off, axis=0)])
    sums = sum_over(sums.reshape(16, 128), "x")
    sums = sum_over(sums, "z").reshape(2, -1)
    count = prior_count.astype(jnp.float32)
    total = count + batch_n
    run_mean = prior_mean + sums[0] / total
    run_var = (prior_var * count + (sums[1] - sums[0] * sums[0] / total)) / total
    scale = 1.0 / jnp.sqrt(run_var + 1e-05)

    blocks = [along_x(observations, by) if by else observations for by in BLOCKS]
    q = jnp.where(c == 0, z - jnp.arange(8), z + 1 + jnp.arange(8)) % 16
    places = (2 * (q % 4) + (q // 4) % 2).astype(jnp.int32)
    order = ((x + jnp.array(BLOCKS)) % 4).astype(jnp.int32)
    value = normal(blocks, run_mean, scale)
    part = product(0, order, places, slots, value)
    value = across(value)
    part = product(1, order, places, slots, value, part)

    part = lax.all_to_all(part.reshape(16, -1, rows), ("x", "y"), 0, 0)
    summed = part.reshape(4, 4, 2, -1, rows).astype(jnp.float32).sum(axis=1)
    summed = summed.astype(jnp.bfloat16)
    other = across(summed)
    sides = []
    for half in range(2):
        q = 4 * (2 * c + half) + y
        mine = jnp.where(c == 0, z - q, q - z - 1) % 16 < 8
        sides.append(jnp.where(mine, summed[:, half], other[:, half]))
    logits = jnp.concatenate(sides, axis=0).reshape(-1, rows).T
    return (run_mean, run_var, logits)


def solution(mesh):
    torus = Mesh(mesh.devices.reshape(SHAPE), AXES)
    in_specs = (P(ENV, FEAT), P(FEAT), P(FEAT), P(FEAT), P(FEAT, ENV))
    out_specs = (P(FEAT), P(FEAT), P(ENV, FEAT))
    return jax.shard_map(step, mesh=torus, in_specs=in_specs, out_specs=out_specs, check_vma=False)
```

```python
import functools

import jax
import jax.numpy as jnp
import numpy as np
from jax import lax
from jax.experimental import pallas as pl
from jax.experimental.pallas import tpu as pltpu
from jax.sharding import Mesh
from jax.sharding import PartitionSpec as P

ENV = ("x", "z")
FEAT = ("y", "c")
SIZES = {"x": 4, "z": 16, "y": 4, "c": 2}
AXES = tuple(SIZES)
SHAPE = tuple(SIZES.values())

BLOCKS = ((0, 1, 3, 2), (0, 3, 1, 2))


def fetch(value, source):
    pairs = []
    for to in range(int(np.prod(SHAPE))):
        at = source(*(int(k) for k in np.unravel_index(to, SHAPE)))
        at = tuple(k % n for k, n in zip(at, SHAPE))
        pairs.append((int(np.ravel_multi_index(at, SHAPE)), to))
    return lax.ppermute(value, AXES, pairs)


def along_x(value, k):
    return fetch(value, lambda x, z, y, c: (x + BLOCKS[c][k], z, y, c))


def holder(x, q):
    q = q % 16
    return q % 4, 4 * (q // 4) + x


def across(value):
    return fetch(value, lambda x, z, y, c: (x, z, y, 1 - c))


def along_z(value, by):
    return fetch(value, lambda x, z, y, c: (x, z + (by if c else -by), y, c))


def sum_over(value, axis):
    copies = jnp.broadcast_to(value[None], (lax.axis_size(axis), *value.shape))
    copies = lax.all_to_all(copies, axis, 0, 0)
    return copies.sum(axis=0)


def normal_kernel(mean, factor, *refs):
    for k, block in enumerate(refs[:-1]):
        value = (block[...].astype(jnp.float32) - mean[...]) * factor[...]
        refs[-1][k] = jnp.clip(value, -5.0, 5.0).astype(jnp.bfloat16)


def normal(blocks, mean, factor):
    rows, depth = blocks[0].shape
    tile = rows // 2
    line = pl.BlockSpec((1, depth), lambda k: (0, 0))
    return pl.pallas_call(
        normal_kernel,
        out_shape=jax.ShapeDtypeStruct((4, rows, depth), jnp.bfloat16),
        grid=(rows // tile,),
        in_specs=[line, line] + [pl.BlockSpec((tile, depth), lambda k: (k, 0))] * 4,
        out_specs=pl.BlockSpec((4, tile, depth), lambda k: (0, k, 0)),
        compiler_params=pltpu.CompilerParams(vmem_limit_bytes=24 * 1024 * 1024),
        cost_estimate=pl.CostEstimate(
            flops=20 * rows * depth, bytes_accessed=16 * rows * depth, transcendentals=0
        ),
    )(mean[None], factor[None], *blocks)


def product_kernel(side, order, places, *refs):
    slots, value = refs[:8], refs[8]
    *before, out, weight, held, sem, held_sem = refs[9:]
    step = pl.program_id(0)
    width = slots[0].shape[0] // 2

    def copy(k):
        return pltpu.make_async_copy(
            slots[k].at[pl.ds(side * width, width)],
            weight.at[pl.ds(pl.multiple_of(places[k] * width, width), width)],
            sem.at[k],
        )

    def fetched(k):
        return pltpu.make_async_copy(value.at[k], held.at[k], held_sem.at[k])

    @pl.when(step == 0)
    def _():
        for k in range(8):
            copy(k).start()
        for k in range(4):
            fetched(k).start()
        for k in range(8):
            copy(k).wait()

    fetched(step).wait()
    total = lax.dot_general(
        weight[...], held[step], (((1,), (1,)), ((), ())), preferred_element_type=jnp.float32
    )
    if before:
        total = total + before[0][0].astype(jnp.float32)
    total = total.astype(out.dtype)
    if before:
        out[:, 0] = total.reshape(out.shape[0], *out.shape[2:])
    else:
        out[0] = total


def product(side, order, places, slots, value, *before):
    _, rows, depth = value.shape
    columns = 4 * slots[0].shape[0]
    turned = lambda k, *_: (k + jnp.where(k == 1, 1, 0) - jnp.where(k == 2, 1, 0), 0, 0)
    shape, block, to = (4, columns, rows), (1, columns, rows), lambda k, *_: (k, 0, 0)
    if before:
        shape, block = (4, 4, columns // 4, rows), (4, 1, columns // 4, rows)
        to = lambda k, order, places: (0, order[k], 0, 0)
    return pl.pallas_call(
        functools.partial(product_kernel, side),
        out_shape=jax.ShapeDtypeStruct(shape, jnp.bfloat16),
        grid_spec=pltpu.PrefetchScalarGridSpec(
            num_scalar_prefetch=2,
            grid=(4,),
            in_specs=[pl.BlockSpec(memory_space=pl.ANY)] * 9
            + [pl.BlockSpec((1, columns, rows), turned)] * len(before),
            out_specs=pl.BlockSpec(block, to),
            scratch_shapes=[
                pltpu.VMEM((columns, depth), jnp.bfloat16),
                pltpu.VMEM(value.shape, jnp.bfloat16),
                pltpu.SemaphoreType.DMA((8,)),
                pltpu.SemaphoreType.DMA((4,)),
            ],
        ),
        compiler_params=pltpu.CompilerParams(vmem_limit_bytes=16 * 1024 * 1024),
        cost_estimate=pl.CostEstimate(
            flops=8 * columns * rows * depth, bytes_accessed=9 << 20, transcendentals=0
        ),
    )(order, places, *slots, value, *before)


def step(observations, prior_count, prior_mean, prior_var, policy_weight):
    rows, _ = observations.shape
    x, z, y, c = (lax.axis_index(a) for a in AXES)
    batch_n = jnp.float32(rows * lax.axis_size(ENV))

    own = policy_weight.T
    slots = [
        jnp.concatenate(
            [
                fetch(own, lambda x, z, y, c: (*holder(x, z + c), y, c)),
                fetch(own, lambda x, z, y, c: (*holder(x, z + c), y, 1 - c)),
            ],
            axis=0,
        )
    ]
    slots.append(along_z(slots[0], 1))
    for k, start in ((2, 0), (3, 1), (4, 2), (5, 3), (6, 4), (7, 5)):
        slots.append(along_z(slots[start], k - start))

    off = observations.astype(jnp.float32) - prior_mean
    sums = jnp.stack([jnp.sum(off, axis=0), jnp.sum(off * off, axis=0)])
    sums = sum_over(sums.reshape(16, 128), "x")
    sums = sum_over(sums, "z").reshape(2, -1)
    count = prior_count.astype(jnp.float32)
    total = count + batch_n
    run_mean = prior_mean + sums[0] / total
    run_var = (prior_var * count + (sums[1] - sums[0] * sums[0] / total)) / total
    scale = 1.0 / jnp.sqrt(run_var + 1e-05)

    blocks = [observations, along_x(observations, 1), along_x(observations, 2)]
    blocks.append(along_x(blocks[1], 1))
    q = jnp.where(c == 0, z - jnp.arange(8), z + 1 + jnp.arange(8)) % 16
    places = (2 * (q % 4) + (q // 4) % 2).astype(jnp.int32)
    order = ((x + jnp.array(BLOCKS)[1 - c]) % 4).astype(jnp.int32)
    value = normal(blocks, run_mean, scale)
    part = product(0, order, places, slots, value)
    value = across(value)
    part = product(1, order, places, slots, value, part)

    part = lax.all_to_all(part.reshape(16, -1, rows), ("y", "x"), 0, 0)
    summed = part.reshape(4, 4, 2, -1, rows).astype(jnp.float32).sum(axis=0)
    summed = summed.astype(jnp.bfloat16)
    other = across(summed)
    sides = []
    for half in range(2):
        q = 4 * (2 * c + half) + y
        mine = jnp.where(c == 0, z - q, q - z - 1) % 16 < 8
        sides.append(jnp.where(mine, summed[:, half], other[:, half]))
    logits = jnp.concatenate(sides, axis=0).reshape(-1, rows).T
    return (run_mean, run_var, logits)


def solution(mesh):
    torus = Mesh(mesh.devices.reshape(SHAPE), AXES)
    in_specs = (P(ENV, FEAT), P(FEAT), P(FEAT), P(FEAT), P(FEAT, ENV))
    out_specs = (P(FEAT), P(FEAT), P(ENV, FEAT))
    return jax.shard_map(step, mesh=torus, in_specs=in_specs, out_specs=out_specs, check_vma=False)
```
